32 devices in a mesh: dp: 8 (over y, x, core), mp: 4 (over z).
Axes of the slice: x: 2, y: 2, z: 4, core: 2. Of those that a mesh axis runs over, the one named last changes fastest.
Arguments:
- inputs: bfloat16 [1024, 6144], P('dp'), may hold values from -6 to 6
- pre_act: bfloat16 [1024, 12288], P('dp', 'mp'), may hold values from -6 to 6
- out_grad: bfloat16 [1024, 6144], P('dp'), may hold values from -6 to 6
- w_in: bfloat16 [6144, 12288], P(None, 'mp'), may hold values from -0.109375 to 0.109375
- w_out: bfloat16 [12288, 6144], P('mp'), may hold values from -0.0546875 to 0.0546875
- master_in: float32 [6144, 12288], P('dp', 'mp'), may hold values from -0.3 to 0.3
- master_out: float32 [12288, 6144], P('mp', 'dp'), may hold values from -0.3 to 0.3
- row_in: float32 [6144], P('dp'), may hold values from 12.8 to 686.08
- col_in: float32 [12288], P('mp'), may hold values from 25 to 128
- row_out: float32 [12288], P('mp'), may hold values from 25.6 to 1372.16
- col_out: float32 [6144], P('dp'), may hold values from 51 to 256
Outputs:
- input_grad: bfloat16 [1024, 6144], P('dp', 'mp')
- new_master_in: float32 [6144, 12288], P('dp', 'mp')
- new_master_out: float32 [12288, 6144], P('mp', 'dp')
The draws below stay inside these ranges and needn't reach their ends.
All inputs are finite; a program needn't handle non-finite values.
Results may differ from the reference program's by a relative error of at most 0.012.
Values may be sent and summed in bfloat16 or wider, within the bound.
A program may use at most 256 MiB of HBM per device.

```python
import math
import jax
import jax.numpy as jnp
from jax import lax

D = 6144
FF = 12288
TOK_DEV = 128
TOKENS = 1024
N_DP = 8


def falling_factor(key, count, high, ratio):
    place = jnp.arange(count, dtype=jnp.float32) / float(count)
    noise = jax.random.uniform(key, (count,), jnp.float32, -0.28, 0.28)
    return high * jnp.exp(-jnp.log(ratio) * place + noise)


def draw_row_in(key, part):
    return falling_factor(jax.random.fold_in(key, 11), D, TOKENS * 0.5, 10.0)


def draw_row_out(key, part):
    return falling_factor(jax.random.fold_in(key, 23), FF, TOKENS * 1.0, 10.0)


def spiked(entries, key, source, target, blocks, factor):
    owner, partner = [(jnp.arange(entries.shape[position]) // (entries.shape[position] // blocks)).reshape([-1 if axis == position else 1 for axis in range(entries.ndim)]) for position in (source, target)]
    chosen = jax.random.permutation(key, blocks)[partner]
    strong = (owner == chosen) | (owner == (partner + blocks // 2) % blocks)
    return jnp.where(strong, factor * entries, entries)


def levels(rng, extent, cuts, least, high):
    loudness, own = 1.0, jax.random.fold_in(rng, 6)
    for position, blocks in cuts:
        heights = jnp.exp(jax.random.uniform(jax.random.fold_in(own, position), (blocks,), jnp.float32, least / len(cuts), high / len(cuts)))
        loudness = loudness * jnp.repeat(heights, extent[position] // blocks).reshape([-1 if axis == position else 1 for axis in range(len(extent))])
    return loudness


def scatter_about(stream_key, extent, width, most, shards=(), held_as=jnp.bfloat16):
    entries = width * jax.random.normal(stream_key, extent, jnp.float32)
    if shards:
        entries = entries * levels(stream_key, extent, shards, -0.22, 0.18)
    return jnp.clip(entries, -most, most).astype(held_as)


def noise_with(rng, dims, deviation, reach, cuts, heavy, held_as=jnp.bfloat16):
    drawn = deviation * jax.random.normal(rng, dims, jnp.float32)
    if cuts:
        drawn = drawn * levels(rng, dims, cuts, -0.22, 0.18)
    return jnp.clip(spiked(drawn, jax.random.fold_in(rng, 3), *heavy), -reach, reach).astype(held_as)


def setup_inputs(seed: int = 0) -> dict:
    keys = jax.random.split(jax.random.key(seed), 12)
    inputs = noise_with(keys[0], (TOKENS, D), 1.0, 6.0, ((0, 8),), (0, 1, 8, 2.0))
    pre_act = scatter_about(keys[1], (TOKENS, FF), 1.0, 6.0, ((0, 8), (1, 4)))
    out_grad = noise_with(keys[2], (TOKENS, D), 1.0, 6.0, ((0, 8),), (0, 1, 8, 2.0))
    w_in = noise_with(keys[3], (D, FF), D ** -0.5, 0.109375, ((1, 4),), (1, 0, 4, 2.0))
    w_out = scatter_about(keys[4], (FF, D), FF ** -0.5, 0.0546875, ((0, 4),))
    master_in = scatter_about(keys[5], (D, FF), 0.05, 0.3, ((0, 8), (1, 4)), jnp.float32)
    master_out = scatter_about(keys[6], (FF, D), 0.05, 0.3, ((0, 4), (1, 8)), jnp.float32)
    row_in = draw_row_in(jax.random.fold_in(keys[11], 71), 0)
    col_in = jnp.clip(jnp.exp(math.log(128.0) - 1.6331544 * jax.random.uniform(keys[8], (FF,), jnp.float32) ** levels(keys[8], (FF,), ((0, 4),), -0.2, 0.2)), 25.0, 128.0)
    row_out = draw_row_out(jax.random.fold_in(keys[11], 71), 0)
    col_out = jnp.clip(jnp.exp(math.log(256.0) - 1.6133518 * jax.random.uniform(keys[10], (D,), jnp.float32) ** levels(keys[10], (D,), ((0, 8),), -0.2, 0.2)), 51.0, 256.0)
    return dict(inputs=inputs, pre_act=pre_act, out_grad=out_grad, w_in=w_in, w_out=w_out, master_in=master_in, master_out=master_out, row_in=row_in, col_in=col_in, row_out=row_out, col_out=col_out)


decay_rate = 0.8
step_size = 0.05
tiny_square = 1e-30

def gelu_parts(pre):
    cumulative = 0.5 * (1.0 + jax.scipy.special.erf(pre * (1.0 / math.sqrt(2.0))))
    density = jnp.exp(-0.5 * pre * pre) * (1.0 / math.sqrt(2.0 * math.pi))
    return (pre * cumulative, cumulative + pre * density)

def adafactor(grad, master, row_state, col_state):
    square = grad * grad + tiny_square
    row_new = decay_rate * row_state + (1.0 - decay_rate) * lax.optimization_barrier(jnp.mean(square, axis=1))
    col_new = decay_rate * col_state + (1.0 - decay_rate) * lax.optimization_barrier(jnp.mean(square, axis=0))
    second = row_new[:, None] * col_new[None, :] / jnp.mean(row_new)
    update = grad / jnp.sqrt(second)
    return master - step_size * update

def reference(inputs, pre_act, out_grad, w_in, w_out, master_in, master_out, row_in, col_in, row_out, col_out):
    active, slope = gelu_parts(pre_act.astype(jnp.float32))
    hidden = active.astype(jnp.bfloat16)
    hid_grad = jnp.dot(out_grad, w_out.T, preferred_element_type=jnp.float32)
    pre_grad = (hid_grad * slope).astype(jnp.bfloat16)
    input_grad = jnp.dot(pre_grad, w_in.T, preferred_element_type=jnp.float32).astype(jnp.bfloat16)

    def group(totals, index):
        begin = (index * TOK_DEV).astype(jnp.int32)
        rows_x = lax.dynamic_slice_in_dim(inputs, begin, TOK_DEV, 0)
        rows_g = lax.dynamic_slice_in_dim(pre_grad, begin, TOK_DEV, 0)
        rows_h = lax.dynamic_slice_in_dim(hidden, begin, TOK_DEV, 0)
        rows_y = lax.dynamic_slice_in_dim(out_grad, begin, TOK_DEV, 0)
        part_in = jnp.dot(rows_x.T, rows_g, preferred_element_type=jnp.float32).astype(jnp.bfloat16)
        part_out = jnp.dot(rows_h.T, rows_y, preferred_element_type=jnp.float32).astype(jnp.bfloat16)
        part_in, part_out = lax.optimization_barrier((part_in, part_out))
        return ((totals[0] + part_in.astype(jnp.float32), totals[1] + part_out.astype(jnp.float32)), None)
    start_sums = (jnp.zeros((D, FF), jnp.float32), jnp.zeros((FF, D), jnp.float32))
    (grad_in, grad_out), _ = lax.scan(group, start_sums, jnp.arange(N_DP, dtype=jnp.int32))
    new_master_in = adafactor(grad_in, master_in, row_in, col_in)
    new_master_out = adafactor(grad_out, master_out, row_out, col_out)
    return (input_grad, new_master_in, new_master_out)
```

```python
import math

import jax
import jax.numpy as jnp
from jax import lax
from jax.sharding import PartitionSpec as P

D = 6144
FF = 12288


decay_rate = 0.8
step_size = 0.05
tiny_square = 1e-30


def gelu_parts(pre):
    cumulative = 0.5 * (1.0 + jax.scipy.special.erf(pre * (1.0 / math.sqrt(2.0))))
    density = jnp.exp(-0.5 * pre * pre) * (1.0 / math.sqrt(2.0 * math.pi))
    return (pre * cumulative, cumulative + pre * density)


def contract_rows(left, right):
    return lax.dot_general(
        left, right, (((0,), (0,)), ((), ())), preferred_element_type=jnp.float32
    )


def scatter_sum(partial, axis):
    size = lax.axis_size(axis)
    me = lax.axis_index(axis)
    width = partial.shape[1] // size
    piece = lambda k: lax.dynamic_slice_in_dim(partial, k * width, width, 1)
    total = piece(me)
    for shift in range(1, size):
        moved = piece(lax.rem(me + shift, size)).astype(jnp.bfloat16)
        got = lax.ppermute(moved, axis, [(i, (i + shift) % size) for i in range(size)])
        total = total + got.astype(jnp.float32)
    return total


def body(
    inputs, pre_act, out_grad, w_in, w_out, master_in, master_out, row_in, col_in, row_out, col_out
):
    active, slope = gelu_parts(pre_act.astype(jnp.float32))
    hidden_all = lax.all_gather(active.astype(jnp.bfloat16), "dp", axis=0, tiled=True)
    out_cols = lax.all_to_all(out_grad, "dp", 1, 0, tiled=True)
    in_cols = lax.all_to_all(inputs, "dp", 1, 0, tiled=True)
    hid_grad = lax.dot_general(
        out_grad, w_out, (((1,), (1,)), ((), ())), preferred_element_type=jnp.float32
    )
    pre_grad = (hid_grad * slope).astype(jnp.bfloat16)
    pre_grad_all = lax.all_gather(pre_grad, "dp", axis=0, tiled=True)
    input_part = lax.dot_general(
        pre_grad, w_in, (((1,), (1,)), ((), ())), preferred_element_type=jnp.float32
    )
    input_grad = scatter_sum(input_part, "mp").astype(jnp.bfloat16)
    grad_out = contract_rows(hidden_all, out_cols)
    grad_in = contract_rows(in_cols, pre_grad_all)
    square_in = grad_in * grad_in + tiny_square
    square_out = grad_out * grad_out + tiny_square
    width_in, width_out, row_out_sum = lax.psum(
        (jnp.sum(square_in, axis=1), jnp.sum(square_out, axis=0), jnp.sum(row_out)), "mp"
    )
    rows_in = decay_rate * row_in + (1.0 - decay_rate) * width_in / FF
    cols_out = decay_rate * col_out + (1.0 - decay_rate) * width_out / FF
    hidden_in, hidden_out, sum_in, sum_out = lax.psum(
        (
            jnp.sum(square_in, axis=0),
            jnp.sum(square_out, axis=1),
            jnp.sum(rows_in),
            jnp.sum(width_out),
        ),
        "dp",
    )
    cols_in = decay_rate * col_in + (1.0 - decay_rate) * hidden_in / D
    rows_out = decay_rate * row_out + (1.0 - decay_rate) * hidden_out / D
    mean_in = sum_in / D
    mean_out = (decay_rate * row_out_sum + (1.0 - decay_rate) * sum_out / D) / FF
    update_in = grad_in / jnp.sqrt(rows_in[:, None] * cols_in[None, :] / mean_in)
    update_out = grad_out / jnp.sqrt(rows_out[:, None] * cols_out[None, :] / mean_out)
    new_master_in = master_in - step_size * update_in
    new_master_out = master_out - step_size * update_out
    return (input_grad, new_master_in, new_master_out)


def solution(mesh):
    in_specs = (
        P("dp", None),
        P("dp", "mp"),
        P("dp", None),
        P(None, "mp"),
        P("mp", None),
        P("dp", "mp"),
        P("mp", "dp"),
        P("dp"),
        P("mp"),
        P("mp"),
        P("dp"),
    )
    out_specs = (P("dp", "mp"), P("dp", "mp"), P("mp", "dp"))
    return jax.shard_map(body, mesh=mesh, in_specs=in_specs, out_specs=out_specs, check_vma=False)
```

```python
import math

import jax
import jax.numpy as jnp
from jax import lax
from jax.experimental.layout import Layout, with_layout_constraint
from jax.sharding import PartitionSpec as P

D = 6144
FF = 12288


decay_rate = 0.8
step_size = 0.05
tiny_square = 1e-30


def gelu_parts(pre):
    cumulative = 0.5 * (1.0 + jax.scipy.special.erf(pre * (1.0 / math.sqrt(2.0))))
    density = jnp.exp(-0.5 * pre * pre) * (1.0 / math.sqrt(2.0 * math.pi))
    return (pre * cumulative, cumulative + pre * density)


def contract_rows(left, right):
    return lax.dot_general(
        left, right, (((0,), (0,)), ((), ())), preferred_element_type=jnp.float32
    )


def scatter_pieces(partial, axis):
    size = lax.axis_size(axis)
    me = lax.axis_index(axis)
    width = partial.shape[1] // size
    piece = lambda k: lax.dynamic_slice_in_dim(partial, k * width, width, 1)
    pieces = [piece(me)]
    for shift in range(1, size):
        moved = piece(lax.rem(me + shift, size)).astype(jnp.bfloat16)
        pieces.append(lax.ppermute(moved, axis, [(i, (i + shift) % size) for i in range(size)]))
    return pieces


def body(
    inputs, pre_act, out_grad, w_in, w_out, master_in, master_out, row_in, col_in, row_out, col_out
):
    active, slope = gelu_parts(pre_act.astype(jnp.float32))
    hidden = active.astype(jnp.bfloat16)
    hidden_all = lax.all_gather(hidden, "dp", axis=0, tiled=True)
    out_grad, _ = lax.optimization_barrier((out_grad, hidden))
    out_cols = lax.all_to_all(out_grad, "dp", 1, 0, tiled=True)
    hid_grad = lax.dot_general(
        out_grad, w_out, (((1,), (1,)), ((), ())), preferred_element_type=jnp.float32
    )
    pre_grad = (hid_grad * slope).astype(jnp.bfloat16)
    pre_grad_all = lax.all_gather(pre_grad, "dp", axis=0, tiled=True)
    input_part = lax.dot_general(
        pre_grad, w_in, (((1,), (1,)), ((), ())), preferred_element_type=jnp.float32
    )
    inputs, input_part = lax.optimization_barrier((inputs, input_part))
    in_cols = lax.all_to_all(inputs, "dp", 1, 0, tiled=True)
    pieces = scatter_pieces(input_part, "mp")

    grad_out = contract_rows(hidden_all, out_cols)
    square_out = grad_out * grad_out + tiny_square
    width_out, row_out_sum = lax.psum((jnp.sum(square_out, axis=0), jnp.sum(row_out)), "mp")
    cols_out = decay_rate * col_out + (1.0 - decay_rate) * width_out / FF
    hidden_out, sum_out = lax.psum((jnp.sum(square_out, axis=1), jnp.sum(width_out)), "dp")
    rows_out = decay_rate * row_out + (1.0 - decay_rate) * hidden_out / D
    mean_out = (decay_rate * row_out_sum + (1.0 - decay_rate) * sum_out / D) / FF
    update_out = grad_out / jnp.sqrt(rows_out[:, None] * cols_out[None, :] / mean_out)
    new_master_out = master_out - step_size * update_out

    pre_grad_all, new_master_out, pieces = lax.optimization_barrier(
        (pre_grad_all, new_master_out, pieces)
    )
    input_grad = sum(piece.astype(jnp.float32) for piece in pieces).astype(jnp.bfloat16)
    grad_in = with_layout_constraint(contract_rows(in_cols, pre_grad_all), Layout((0, 1)))
    square_in = grad_in * grad_in + tiny_square
    width_in = lax.psum(jnp.sum(square_in, axis=1), "mp")
    rows_in = decay_rate * row_in + (1.0 - decay_rate) * width_in / FF
    hidden_in, sum_in = lax.psum((jnp.sum(square_in, axis=0), jnp.sum(rows_in)), "dp")
    cols_in = decay_rate * col_in + (1.0 - decay_rate) * hidden_in / D
    mean_in = sum_in / D
    update_in = grad_in / jnp.sqrt(rows_in[:, None] * cols_in[None, :] / mean_in)
    new_master_in = master_in - step_size * update_in
    return (input_grad, new_master_in, new_master_out)


def solution(mesh):
    in_specs = (
        P("dp", None),
        P("dp", "mp"),
        P("dp", None),
        P(None, "mp"),
        P("mp", None),
        P("dp", "mp"),
        P("mp", "dp"),
        P("dp"),
        P("mp"),
        P("mp"),
        P("dp"),
    )
    out_specs = (P("dp", "mp"), P("dp", "mp"), P("mp", "dp"))
    return jax.shard_map(body, mesh=mesh, in_specs=in_specs, out_specs=out_specs, check_vma=False)
```
